8 devices in a mesh: dp: 2 (over z, y), ep: 4 (over x, core).
Axes of the slice: x: 2, y: 2, z: 1, core: 2. Of those that a mesh axis runs over, the one named last changes fastest.
Arguments:
- dispatched: bfloat16 [8, 32, 64, 1024], P('dp', 'ep'), parts along dimension 0
- w_gate: bfloat16 [32, 1024, 512], P('ep')
- w_up: bfloat16 [32, 1024, 512], P('ep')
- w_down: bfloat16 [32, 512, 1024], P('ep')
- fill_count: int32 [8, 32], P('dp', 'ep'), parts along dimension 0
- slot_index: int32 [1024, 8], P(('dp', 'ep')), parts along dimension 0
- expert_id: int32 [1024, 8], P(('dp', 'ep')), parts along dimension 0
- gate_weight: float32 [1024, 8], P(('dp', 'ep')), parts along dimension 0
Outputs:
- output: bfloat16 [1024, 1024], P(('dp', 'ep')), parts along dimension 0
There are 2 independent parts. The reference program is written for one: setup_inputs(seed, part) draws one part's arguments, and reference() takes and returns one part's arrays. A program takes and returns all parts, laid end to end along the dimension named above; an argument that names none is the same for every part.
All inputs are finite; a program needn't handle non-finite values.
Results may differ from the reference program's by a relative error of at most 0.001.
Values are sent between devices in bfloat16 or wider.
A program may use at most 1 GiB of HBM per device.

```python
import jax
import jax.numpy as jnp
from jax import lax

HIDDEN = 1024
FFN_DIM = 512
EXPERTS = 32
TOP_K = 8
TOKENS_DEV = 128
GROUP_SIZE = 4
CAPACITY = (2 * TOKENS_DEV * TOP_K) // EXPERTS


def draw_routing(route_key):
    key_perm, key_noise, key_shift = jax.random.split(route_key, 3)
    popularity = jax.random.permutation(key_perm, EXPERTS)
    base_score = 4000 // (popularity + 1)
    noise_term = jax.random.randint(key_noise, (GROUP_SIZE, TOKENS_DEV, EXPERTS), 0, 1000)
    cover_shift = jax.random.randint(key_shift, (GROUP_SIZE, 1), 0, EXPERTS)
    expert_ids = jnp.arange(EXPERTS, dtype=jnp.int32)
    cover_id = (jnp.arange(TOKENS_DEV, dtype=jnp.int32)[None, :] + cover_shift) % EXPERTS
    cover_bonus = jnp.where(expert_ids[None, None, :] == cover_id[:, :, None], 100000, 0)
    route_score = (base_score[None, None, :] + noise_term + cover_bonus) * EXPERTS + expert_ids
    chosen = lax.top_k(route_score, TOP_K)[1]
    onehot = (chosen.reshape(GROUP_SIZE, TOKENS_DEV * TOP_K, 1) == expert_ids).astype(jnp.int32)
    earlier = jnp.cumsum(onehot, axis=1) - onehot
    arrival = jnp.sum(earlier * onehot, axis=2)
    slot_index = jnp.where(arrival < CAPACITY, arrival, -1)
    filled_count = jnp.minimum(jnp.sum(onehot, axis=1), CAPACITY)
    expert_id = chosen.reshape(GROUP_SIZE * TOKENS_DEV, TOP_K).astype(jnp.int32)
    slot_index = slot_index.reshape(GROUP_SIZE * TOKENS_DEV, TOP_K).astype(jnp.int32)
    return expert_id, slot_index, filled_count.astype(jnp.int32)


def setup_inputs(seed: int = 0, part: int = 0) -> dict:
    shared_key, part_root = jax.random.split(jax.random.key(seed))
    key_gate_w, key_up_w, key_down_w = jax.random.split(shared_key, 3)
    part_key = jax.random.fold_in(part_root, part)
    key_route, key_rows, key_mix = jax.random.split(part_key, 3)
    expert_id, slot_index, filled_count = draw_routing(key_route)
    dispatched = jax.random.normal(key_rows, (GROUP_SIZE, EXPERTS, CAPACITY, HIDDEN), jnp.float32)
    w_gate = jax.random.normal(key_gate_w, (EXPERTS, HIDDEN, FFN_DIM), jnp.float32) * HIDDEN ** -0.5
    w_up = jax.random.normal(key_up_w, (EXPERTS, HIDDEN, FFN_DIM), jnp.float32) * HIDDEN ** -0.5
    w_down = jax.random.normal(key_down_w, (EXPERTS, FFN_DIM, HIDDEN), jnp.float32) * FFN_DIM ** -0.5
    logits = jax.random.normal(key_mix, (GROUP_SIZE * TOKENS_DEV, TOP_K), jnp.float32) * 1.5
    return {
        "dispatched": dispatched.astype(jnp.bfloat16),
        "w_gate": w_gate.astype(jnp.bfloat16),
        "w_up": w_up.astype(jnp.bfloat16),
        "w_down": w_down.astype(jnp.bfloat16),
        "fill_count": filled_count,
        "slot_index": slot_index,
        "expert_id": expert_id,
        "gate_weight": jax.nn.softmax(logits, axis=-1),
    }


def reference(dispatched, w_gate, w_up, w_down, fill_count, slot_index, expert_id, gate_weight):
    group_size = dispatched.shape[0]
    capacity = dispatched.shape[2]
    tokens_dev = slot_index.shape[0] // group_size

    def expert_ffn(operands):
        row_block, gate_w, up_w, down_w, filled = operands
        rows_f32 = row_block.astype(jnp.float32)
        pre_gate = jnp.einsum("scd,df->scf", rows_f32, gate_w.astype(jnp.float32))
        pre_up = jnp.einsum("scd,df->scf", rows_f32, up_w.astype(jnp.float32))
        hidden = (jax.nn.silu(pre_gate) * pre_up).astype(jnp.bfloat16)
        result = jnp.einsum("scf,fd->scd", hidden.astype(jnp.float32), down_w.astype(jnp.float32)).astype(jnp.bfloat16)
        live_mask = jnp.arange(capacity)[None, :] < filled[:, None]
        return jnp.where(live_mask[:, :, None], result, jnp.zeros_like(result))

    expert_out = lax.map(expert_ffn, (jnp.swapaxes(dispatched, 0, 1), w_gate, w_up, w_down, jnp.swapaxes(fill_count, 0, 1)))
    flat_rows = expert_out.reshape(-1, expert_out.shape[-1])
    source = (jnp.arange(slot_index.shape[0]) // tokens_dev)[:, None]
    row_index = (expert_id * group_size + source) * capacity + jnp.maximum(slot_index, 0)
    weight = jnp.where(slot_index >= 0, gate_weight, 0.0)
    combined = jnp.zeros((slot_index.shape[0], flat_rows.shape[1]), jnp.float32)
    for choice in range(slot_index.shape[1]):
        picked = jnp.take(flat_rows, row_index[:, choice], axis=0).astype(jnp.float32)
        combined = combined + weight[:, choice, None] * picked
    return combined.astype(jnp.bfloat16)
```

```python
import functools

import jax
import jax.numpy as jnp
from jax import lax
from jax.experimental import pallas as pl
from jax.experimental.pallas import tpu as pltpu
from jax.sharding import PartitionSpec as P

MESH = pl.DeviceIdType.MESH
LOOKAHEAD = 3
CHUNK = 256
BF16_MAX = 3.3895313892515355e38


def split3(value):
    high = jnp.minimum(value, BF16_MAX).astype(jnp.bfloat16)
    rest = value - high.astype(jnp.float32)
    middle = rest.astype(jnp.bfloat16)
    low = (rest - middle.astype(jnp.float32)).astype(jnp.bfloat16)
    return jnp.concatenate([high, middle, low], axis=0)


def kernel(x_hbm, wg_hbm, wu_hbm, wd_hbm, fill_hbm, slot_hbm, expert_hbm, gate_hbm, out_hbm,
           x_buf, wg_buf, wu_buf, wd_buf, fill_buf, slot_buf, expert_buf, gate_buf,
           route_out, route_in, mix, hid, rows_buf, give_buf, keep_buf, from_peer, link_out, link_in, out_buf,
           x_sem, wg_sem, wu_sem, wd_sem, small_sem, out_sem,
           route_send, route_recv, give_send, give_recv, link_send, link_recv):
    experts, width, ffn = wg_hbm.shape
    capacity = x_hbm.shape[2]
    tokens = slot_hbm.shape[1]
    choices = slot_hbm.shape[0]
    chunks = width // CHUNK
    group = lax.axis_index("dp")
    me = lax.axis_index("ep")
    core = lax.rem(me, 2)
    chip = me // 2
    partner = chip * 2 + (1 - core)
    far = (1 - chip) * 2 + core
    far_other = (1 - chip) * 2 + (1 - core)
    sources = (far_other, far, partner, me)

    def x_copy(role, e):
        return pltpu.make_async_copy(
            x_hbm.at[sources[role], e], x_buf.at[e, pl.ds(role * capacity, capacity)], x_sem.at[role, e])

    def wg_copy(e):
        return pltpu.make_async_copy(wg_hbm.at[e], wg_buf.at[e], wg_sem.at[e])

    def wu_copy(e):
        return pltpu.make_async_copy(wu_hbm.at[e], wu_buf.at[e], wu_sem.at[e])

    def wd_copy(n):
        cols = pl.ds(pl.multiple_of(n * CHUNK, CHUNK), CHUNK)
        return pltpu.make_async_copy(wd_hbm.at[:, :, cols], wd_buf.at[:, :, cols], wd_sem.at[n])

    def start_expert(e):
        x_copy(0, e).start()
        x_copy(1, e).start()
        wg_copy(e).start()
        wu_copy(e).start()

    small = [pltpu.make_async_copy(src, dst, small_sem.at[i]) for i, (src, dst) in enumerate(
        ((slot_hbm, slot_buf), (expert_hbm, expert_buf), (gate_hbm, gate_buf), (fill_hbm, fill_buf)))]
    for copy in small:
        copy.start()
    for e in range(LOOKAHEAD):
        start_expert(e)

    barrier = pltpu.get_barrier_semaphore()
    for peer in (partner, far, far_other):
        pl.semaphore_signal(barrier, inc=1, device_id=(group, peer), device_id_type=MESH)

    for copy in small:
        copy.wait()
    slot = slot_buf[...]
    code = jnp.where(slot >= 0, expert_buf[...] * capacity + slot, -1)
    route_out[0:choices] = code.astype(jnp.float32)
    route_out[choices:] = gate_buf[...]

    pl.semaphore_wait(barrier, 3)
    route_copies = [
        pltpu.make_async_remote_copy(
            src_ref=route_out, dst_ref=route_in.at[role], send_sem=route_send.at[role],
            recv_sem=route_recv.at[role], device_id=(group, peer), device_id_type=MESH)
        for role, peer in ((0, far_other), (1, far), (2, partner))]
    for copy in route_copies:
        copy.start()

    def hidden(first, e):
        rows = x_buf[e, pl.ds(first * capacity, 2 * capacity)]
        pre_gate = jnp.dot(rows, wg_buf[e], preferred_element_type=jnp.float32)
        pre_up = jnp.dot(rows, wu_buf[e], preferred_element_type=jnp.float32)
        value = jax.nn.silu(pre_gate) * pre_up
        row = lax.broadcasted_iota(jnp.int32, value.shape, 0)
        limit = jnp.where(row < capacity, fill_buf[sources[first], e], fill_buf[sources[first + 1], e] + capacity)
        hid[e, pl.ds(first * capacity, 2 * capacity)] = jnp.where(row < limit, value, 0.0).astype(jnp.bfloat16)

    def remote_step(e, carry):
        wg_copy(e).wait()
        wu_copy(e).wait()
        x_copy(0, e).wait()
        x_copy(1, e).wait()

        @pl.when(e + LOOKAHEAD < experts)
        def _():
            start_expert(e + LOOKAHEAD)

        @pl.when(e + LOOKAHEAD >= experts)
        def _():
            wd_copy(e + LOOKAHEAD - experts).start()

        hidden(0, e)
        return carry

    lax.fori_loop(0, experts, remote_step, 0)
    for n in range(LOOKAHEAD, chunks):
        wd_copy(n).start()
    for role in (2, 3):
        for e in range(experts):
            x_copy(role, e).start()

    def build_mix(role):
        route = route_out if role == 3 else route_in.at[role]
        code = route[0:choices].astype(jnp.int32)
        gate = route[choices:]
        row = lax.broadcasted_iota(jnp.int32, (experts * capacity, tokens), 0) + me * (experts * capacity)
        value = jnp.zeros((experts * capacity, tokens), jnp.float32)
        for j in range(choices):
            value = jnp.where(row == code[j:j + 1], gate[j:j + 1], value)
        mix[role] = split3(value.T)

    def rows_of(first, n):
        cols = pl.ds(n * CHUNK, CHUNK)
        for e in range(experts):
            value = jnp.dot(hid[e, pl.ds(first * capacity, 2 * capacity)], wd_buf[e, :, cols],
                            preferred_element_type=jnp.float32).astype(jnp.bfloat16)
            rows_buf[0, pl.ds(e * capacity, capacity)] = value[:capacity]
            rows_buf[1, pl.ds(e * capacity, capacity)] = value[capacity:]

    def mixed(role):
        value = jnp.dot(mix[role], rows_buf[role % 2], preferred_element_type=jnp.float32)
        return value[:tokens] + value[tokens:2 * tokens] + value[2 * tokens:]

    def give_copy(kind, n):
        return pltpu.make_async_remote_copy(
            src_ref=give_buf.at[kind, n], dst_ref=from_peer.at[kind, n], send_sem=give_send.at[kind, n],
            recv_sem=give_recv.at[kind, n], device_id=(group, partner), device_id_type=MESH)

    def link_copy(n):
        return pltpu.make_async_remote_copy(
            src_ref=link_out.at[n], dst_ref=link_in.at[n], send_sem=link_send.at[n],
            recv_sem=link_recv.at[n], device_id=(group, far), device_id_type=MESH)

    def send_on(n):
        give_copy(0, n).wait_recv()
        link_out[n] = keep_buf[0, n] + from_peer[0, n]
        link_copy(n).start()

    for role in (0, 1):
        route_copies[role].wait_recv()
        build_mix(role)
    for n in range(chunks):
        wd_copy(n).wait()
        rows_of(0, n)
        give_buf[0, n] = mixed(0)
        give_copy(0, n).start()
        keep_buf[0, n] = mixed(1)
        if n >= 1:
            send_on(n - 1)

    def local_step(e, carry):
        x_copy(2, e).wait()
        x_copy(3, e).wait()
        hidden(2, e)
        return carry

    lax.fori_loop(0, 2, local_step, 0)
    send_on(chunks - 1)
    lax.fori_loop(2, experts, local_step, 0)
    route_copies[2].wait_recv()
    for role in (2, 3):
        build_mix(role)
    for n in range(chunks):
        rows_of(2, n)
        give_buf[1, n] = mixed(2)
        give_copy(1, n).start()
        keep_buf[1, n] = mixed(3)

    for n in range(chunks):
        give_copy(1, n).wait_recv()
        near = keep_buf[1, n] + from_peer[1, n]
        link_copy(n).wait_recv()
        cols = pl.ds(n * CHUNK, CHUNK)
        out_buf[:, cols] = (near + link_in[n]).astype(jnp.bfloat16)
        pltpu.make_async_copy(out_buf.at[:, cols], out_hbm.at[:, cols], out_sem.at[n]).start()
    for n in range(chunks):
        cols = pl.ds(n * CHUNK, CHUNK)
        pltpu.make_async_copy(out_buf.at[:, cols], out_hbm.at[:, cols], out_sem.at[n]).wait()
        for kind in range(2):
            give_copy(kind, n).wait_send()
        link_copy(n).wait_send()
    for copy in route_copies:
        copy.wait_send()


def solution(mesh):
    def local_step(dispatched, w_gate, w_up, w_down, fill_count, slot_index, expert_id, gate_weight):
        sources, experts, capacity, width = dispatched.shape
        ffn = w_gate.shape[2]
        tokens, choices = slot_index.shape
        chunks = width // CHUNK
        f32, bf16 = jnp.float32, jnp.bfloat16
        any_spec = pl.BlockSpec(memory_space=pl.ANY)
        scratch = [
            pltpu.VMEM((experts, sources * capacity, width), bf16),
            pltpu.VMEM((experts, width, ffn), bf16),
            pltpu.VMEM((experts, width, ffn), bf16),
            pltpu.VMEM((experts, ffn, width), bf16),
            pltpu.SMEM((sources, experts), jnp.int32),
            pltpu.VMEM((choices, tokens), jnp.int32),
            pltpu.VMEM((choices, tokens), jnp.int32),
            pltpu.VMEM((choices, tokens), f32),
            pltpu.VMEM((2 * choices, tokens), f32),
            pltpu.VMEM((3, 2 * choices, tokens), f32),
            pltpu.VMEM((4, 3 * tokens, experts * capacity), bf16),
            pltpu.VMEM((experts, sources * capacity, ffn), bf16),
            pltpu.VMEM((2, experts * capacity, CHUNK), bf16),
            pltpu.VMEM((2, chunks, tokens, CHUNK), f32),
            pltpu.VMEM((2, chunks, tokens, CHUNK), f32),
            pltpu.VMEM((2, chunks, tokens, CHUNK), f32),
            pltpu.VMEM((chunks, tokens, CHUNK), f32),
            pltpu.VMEM((chunks, tokens, CHUNK), f32),
            pltpu.VMEM((tokens, width), bf16),
            pltpu.SemaphoreType.DMA((4, experts)),
            pltpu.SemaphoreType.DMA((experts,)),
            pltpu.SemaphoreType.DMA((experts,)),
            pltpu.SemaphoreType.DMA((chunks,)),
            pltpu.SemaphoreType.DMA((4,)),
            pltpu.SemaphoreType.DMA((chunks,)),
            pltpu.SemaphoreType.DMA((3,)),
            pltpu.SemaphoreType.DMA((3,)),
            pltpu.SemaphoreType.DMA((2, chunks)),
            pltpu.SemaphoreType.DMA((2, chunks)),
            pltpu.SemaphoreType.DMA((chunks,)),
            pltpu.SemaphoreType.DMA((chunks,)),
        ]
        return pl.pallas_call(
            kernel,
            out_shape=jax.ShapeDtypeStruct((tokens, width), bf16),
            in_specs=[any_spec] * 8,
            out_specs=any_spec,
            scratch_shapes=scratch,
            compiler_params=pltpu.CompilerParams(
                collective_id=0, has_side_effects=True, vmem_limit_bytes=60 * 1024 * 1024),
            name="expert_return",
        )(dispatched, w_gate, w_up, w_down, fill_count, slot_index.T, expert_id.T, gate_weight.T)

    token_spec = P(("dp", "ep"))
    in_specs = (P("dp", "ep"), P("ep"), P("ep"), P("ep"), P("dp", "ep"), token_spec, token_spec, token_spec)
    return jax.shard_map(local_step, mesh=mesh, in_specs=in_specs, out_specs=token_spec, check_vma=False)
```

```python
import jax
import jax.numpy as jnp
from jax import lax
from jax.experimental import pallas as pl
from jax.experimental.pallas import tpu as pltpu
from jax.sharding import PartitionSpec as P

MESH = pl.DeviceIdType.MESH
RING = 3
CHUNK = 256
DIRECT = 48
BF16_MAX = 3.3895313892515355e38


def split3(value):
    high = jnp.minimum(value, BF16_MAX).astype(jnp.bfloat16)
    rest = value - high.astype(jnp.float32)
    middle = rest.astype(jnp.bfloat16)
    low = (rest - middle.astype(jnp.float32)).astype(jnp.bfloat16)
    return jnp.concatenate([high, middle, low], axis=0)


def kernel(x_hbm, wg_hbm, wu_hbm, wd_hbm, fill_hbm, slot_hbm, expert_hbm, gate_hbm, out_ref,
           x_buf, w_buf, wd_buf, fill_buf, id_buf, gate_buf,
           route_out, route_in, mix, hid, rows_buf, sums, from_peer, link_out, link_in, direct_in,
           w_sem, x_sem, small_sem, route_send, route_recv, give_send, give_recv, link_send, link_recv,
           direct_send, rest_send, side_recv):
    experts = wg_hbm.shape[0]
    capacity, width = x_hbm.shape[2:]
    choices, tokens = slot_hbm.shape
    chunks = width // CHUNK
    pair = 2 * capacity
    half = experts // 2
    group = lax.axis_index("dp")
    me = lax.axis_index("ep")
    core = lax.rem(me, 2)
    chip = me // 2
    partner = chip * 2 + (1 - core)
    far = (1 - chip) * 2 + core
    far_other = (1 - chip) * 2 + (1 - core)
    sources = (far_other, far, partner, me)

    def start_expert(e):
        for role in range(2):
            pltpu.make_async_copy(
                x_hbm.at[sources[role], e], x_buf.at[e, pl.ds(role * capacity, capacity)],
                x_sem.at[lax.rem(e, RING)]).start()
        for i, src in enumerate((wg_hbm, wu_hbm)):
            pltpu.make_async_copy(src.at[e], w_buf.at[e, i], w_sem.at[lax.rem(e, RING)]).start()

    def start_step(e, carry):
        start_expert(e)
        return carry

    def early_down_copy(e):
        return pltpu.make_async_copy(
            wd_hbm.at[e, :, pl.ds(0, CHUNK)], wd_buf.at[e, :, pl.ds(0, CHUNK)], x_sem.at[lax.rem(e + half, RING)])

    def wait_expert(e, late):
        part = x_buf.at[e] if late else x_buf.at[e, pl.ds(0, pair)]
        pltpu.make_async_copy(part, part, x_sem.at[lax.rem(e, RING)]).wait()
        pltpu.make_async_copy(w_buf.at[e], w_buf.at[e], w_sem.at[lax.rem(e, RING)]).wait()

    def down_copy(n):
        some = pl.ds(half, half) if n == 0 else pl.ds(0, experts)
        cols = pl.ds(n * CHUNK, CHUNK)
        return pltpu.make_async_copy(
            wd_hbm.at[some, :, cols], wd_buf.at[some, :, cols], w_sem.at[(experts + n) % RING])

    small = [pltpu.make_async_copy(src, dst, small_sem.at[i]) for i, (src, dst) in enumerate(
        ((slot_hbm, id_buf.at[0]), (expert_hbm, id_buf.at[1]), (gate_hbm, gate_buf), (fill_hbm, fill_buf)))]
    for copy in small:
        copy.start()
    lax.fori_loop(0, RING, start_step, 0)

    barrier = pltpu.get_barrier_semaphore()
    for peer in (partner, far, far_other):
        pl.semaphore_signal(barrier, inc=1, device_id=(group, peer), device_id_type=MESH)

    for copy in small:
        copy.wait()
    slot = id_buf[0]
    code = jnp.where(slot >= 0, id_buf[1] * capacity + slot, -1)
    route_out[0:choices] = code.astype(jnp.float32)
    route_out[choices:] = gate_buf[...]

    with jax.named_scope("bar"):
        pl.semaphore_wait(barrier, 3)
    for role, peer in ((0, far_other), (1, far), (2, partner)):
        pltpu.make_async_remote_copy(
            src_ref=route_out, dst_ref=route_in.at[role], send_sem=route_send, recv_sem=route_recv,
            device_id=(group, peer), device_id_type=MESH).start()

    def route_all(src, dst):
        return pltpu.make_async_remote_copy(
            src_ref=route_in, dst_ref=route_in, send_sem=route_send, recv_sem=route_recv,
            device_id=(group, partner), device_id_type=MESH)

    def hidden(first, e):
        rows = x_buf[e, pl.ds(first * capacity, pair)]
        pre_gate = jnp.dot(rows, w_buf[e, 0], preferred_element_type=jnp.float32)
        pre_up = jnp.dot(rows, w_buf[e, 1], preferred_element_type=jnp.float32)
        value = jax.nn.silu(pre_gate) * pre_up
        row = lax.broadcasted_iota(jnp.int32, value.shape, 0)
        limit = jnp.where(row < capacity, fill_buf[sources[first], e], fill_buf[sources[first + 1], e] + capacity)
        hid[e, pl.ds(first * capacity, pair)] = jnp.where(row < limit, value, 0.0).astype(jnp.bfloat16)

    def first_step(e, carry):
        with jax.named_scope("w_e"):
            wait_expert(e, False)

        @pl.when(e + RING >= half)
        def _():
            early_down_copy(e + RING - half).start()

        start_expert(e + RING)
        with jax.named_scope("hid"):
            hidden(0, e)
        return carry

    def late_step(e, carry):
        with jax.named_scope("w_e"):
            wait_expert(e, True)

        @pl.when(e + RING < experts)
        def _():
            early_down_copy(e + RING - half).start()
            start_expert(e + RING)

        for n in range(RING):
            @pl.when(e + RING == experts + n)
            def _():
                down_copy(n).start()

        with jax.named_scope("hid"):
            rows_of(0, 0, e - half)
            hidden(0, e)
        return carry

    def build_mix(role):
        route = route_out if role == 3 else route_in.at[role]
        code = route[0:choices].astype(jnp.int32)
        gate = route[choices:]
        row = lax.broadcasted_iota(jnp.int32, (experts * capacity, tokens), 0) + me * (experts * capacity)
        value = jnp.zeros((experts * capacity, tokens), jnp.float32)
        for j in range(choices):
            value = jnp.where(row == code[j:j + 1], gate[j:j + 1], value)
        value = value.T
        block = tokens // 2
        mix[role, 0:3 * block] = split3(value[:block])
        mix[role, 3 * block:] = split3(value[block:])

    def rows_of(first, n, e):
        value = jnp.dot(hid[e, pl.ds(first * capacity, pair)], wd_buf[e, :, pl.ds(n * CHUNK, CHUNK)],
                        preferred_element_type=jnp.float32).astype(jnp.bfloat16)
        here = pl.ds(e * capacity, capacity)
        rows_buf[0, here] = value[:capacity]
        rows_buf[1, here] = value[capacity:]

    def mixed(role):
        block = tokens // 2
        parts = []
        for part in range(2):
            value = jnp.dot(mix[role, pl.ds(part * 3 * block, 3 * block)], rows_buf[role % 2],
                            preferred_element_type=jnp.float32)
            parts.append(value[:block] + value[block:2 * block] + value[2 * block:])
        return jnp.concatenate(parts, axis=0)

    def give_copy(kind, n):
        return pltpu.make_async_remote_copy(
            src_ref=sums.at[kind, 0, n], dst_ref=from_peer.at[kind, n], send_sem=give_send,
            recv_sem=give_recv.at[n if kind == 0 else chunks], device_id=(group, partner), device_id_type=MESH)

    direct_copy = pltpu.make_async_remote_copy(
        src_ref=sums.at[0, 1 - core, 0, pl.ds(0, DIRECT)], dst_ref=direct_in.at[core], send_sem=direct_send,
        recv_sem=side_recv, device_id=(group, (1 - chip) * 2), device_id_type=MESH)
    rest_copy = pltpu.make_async_remote_copy(
        src_ref=link_out.at[0, pl.ds(0, DIRECT)], dst_ref=link_in.at[0, pl.ds(0, DIRECT)], send_sem=rest_send,
        recv_sem=side_recv, device_id=(group, far), device_id_type=MESH)

    def link_copy(n):
        part = pl.ds(DIRECT, tokens - DIRECT) if n == 0 else pl.ds(0, tokens)
        return pltpu.make_async_remote_copy(
            src_ref=link_out.at[n, part], dst_ref=link_in.at[n, part], send_sem=link_send,
            recv_sem=link_recv.at[n], device_id=(group, far), device_id_type=MESH)

    def send_on(n):
        give_copy(0, n).wait_recv()
        link_out[n] = sums[0, 1, n] + from_peer[0, n]
        if n == 0:
            @pl.when(core == 1)
            def _():
                rest_copy.start()
        link_copy(n).start()

    lax.fori_loop(0, half, first_step, 0)
    with jax.named_scope("w_route"):
        route_all(0, 0).wait_recv()
    with jax.named_scope("mix"):
        build_mix(0)
    lax.fori_loop(half, half + 2, late_step, 0)
    with jax.named_scope("mix"):
        build_mix(1)
    lax.fori_loop(half + 2, experts, late_step, 0)

    for n in range(chunks):
        with jax.named_scope("w_d"):
            down_copy(n).wait()
        if n + RING < chunks:
            down_copy(n + RING).start()
        if n == 0:
            for role in (2, 3):
                pltpu.make_async_copy(
                    x_hbm.at[sources[role]], x_buf.at[:, pl.ds(role * capacity, capacity)], small_sem.at[0]).start()
        with jax.named_scope("rows"):
            for e in range(half if n == 0 else 0, experts):
                rows_of(0, n, e)
        with jax.named_scope("mixed"):
            sums[0, 0, n] = mixed(0)
            if n == 0:
                give_copy(0, n).start()

                @pl.when(core == 1)
                def _():
                    direct_copy.start()
            sums[0, 1, n] = mixed(1)
            if n == 0:
                @pl.when(core == 0)
                def _():
                    direct_copy.start()
            else:
                give_copy(0, n).start()
        with jax.named_scope("send_on"):
            if n == 0:
                send_on(n)
            if n >= 2:
                send_on(n - 1)

    local_rows = x_buf.at[:, pl.ds(pair, pair)]
    pltpu.make_async_copy(local_rows, local_rows, small_sem.at[0]).wait()

    def local_step(e, carry):
        hidden(2, e)
        return carry

    lax.fori_loop(0, 2, local_step, 0)
    send_on(chunks - 1)
    with jax.named_scope("phase1L"):
        lax.fori_loop(2, experts, local_step, 0)
    for role in (2, 3):
        build_mix(role)
    for n in range(chunks):
        with jax.named_scope("rows2"):
            for e in range(experts):
                rows_of(2, n, e)
        with jax.named_scope("mixed2"):
            sums[1, 0, n] = mixed(2)
            sums[1, 1, n] = mixed(3)
            give_copy(1, n).start()

    with jax.named_scope("fin_give"):
        pltpu.make_async_remote_copy(
            src_ref=sums.at[1, 0], dst_ref=from_peer.at[1], send_sem=give_send, recv_sem=give_recv.at[chunks],
            device_id=(group, partner), device_id_type=MESH).wait_recv()

    with jax.named_scope("fin_side"):
        @pl.when(core == 0)
        def _():
            pltpu.make_async_remote_copy(
                src_ref=direct_in, dst_ref=direct_in, send_sem=direct_send, recv_sem=side_recv,
                device_id=(group, far), device_id_type=MESH).wait_recv()
            link_in[0, 0:DIRECT] = direct_in[0] + direct_in[1]

        @pl.when(core == 1)
        def _():
            rest_copy.wait_recv()

    for n in range(chunks):
        near = sums[1, 1, n] + from_peer[1, n]
        with jax.named_scope("fin_link"):
            link_copy(n).wait_recv()
        out_ref[:, pl.ds(n * CHUNK, CHUNK)] = (near + link_in[n]).astype(jnp.bfloat16)

    with jax.named_scope("w_send"):
        all_given = sums.at[:, 0]
        pltpu.make_async_remote_copy(
            src_ref=all_given, dst_ref=from_peer, send_sem=give_send, recv_sem=give_recv.at[chunks],
            device_id=(group, partner), device_id_type=MESH).wait_send()
        sent = link_out.at[pl.ds(0, chunks - 1)]
        first = link_out.at[0, pl.ds(DIRECT, tokens - DIRECT)]
        for part in (sent, first):
            pltpu.make_async_remote_copy(
                src_ref=part, dst_ref=part, send_sem=link_send, recv_sem=link_recv.at[0],
                device_id=(group, far), device_id_type=MESH).wait_send()
        direct_copy.wait_send()

        @pl.when(core == 1)
        def _():
            rest_copy.wait_send()
        route_all(0, 0).wait_send()


def solution(mesh):
    def local_step(dispatched, w_gate, w_up, w_down, fill_count, slot_index, expert_id, gate_weight):
        sources, experts, capacity, width = dispatched.shape
        ffn = w_gate.shape[2]
        tokens, choices = slot_index.shape
        chunks = width // CHUNK
        f32, bf16 = jnp.float32, jnp.bfloat16
        scratch = [
            pltpu.VMEM((experts, sources * capacity, width), bf16),
            pltpu.VMEM((experts, 2, width, ffn), bf16),
            pltpu.VMEM((experts, ffn, width), bf16),
            pltpu.SMEM((sources, experts), jnp.int32),
            pltpu.VMEM((2, choices, tokens), jnp.int32),
            pltpu.VMEM((choices, tokens), f32),
            pltpu.VMEM((2 * choices, tokens), f32),
            pltpu.VMEM((3, 2 * choices, tokens), f32),
            pltpu.VMEM((4, 3 * tokens, experts * capacity), bf16),
            pltpu.VMEM((experts, sources * capacity, ffn), bf16),
            pltpu.VMEM((2, experts * capacity, CHUNK), bf16),
            pltpu.VMEM((2, 2, chunks, tokens, CHUNK), f32),
            pltpu.VMEM((2, chunks, tokens, CHUNK), f32),
            pltpu.VMEM((chunks, tokens, CHUNK), f32),
            pltpu.VMEM((chunks, tokens, CHUNK), f32),
            pltpu.VMEM((2, DIRECT, CHUNK), f32),
            pltpu.SemaphoreType.DMA((RING,)),
            pltpu.SemaphoreType.DMA((RING,)),
            pltpu.SemaphoreType.DMA((4,)),
            pltpu.SemaphoreType.DMA,
            pltpu.SemaphoreType.DMA,
            pltpu.SemaphoreType.DMA,
            pltpu.SemaphoreType.DMA((chunks + 1,)),
            pltpu.SemaphoreType.DMA,
            pltpu.SemaphoreType.DMA((chunks,)),
            pltpu.SemaphoreType.DMA,
            pltpu.SemaphoreType.DMA,
            pltpu.SemaphoreType.DMA,
        ]
        operands = (dispatched, w_gate, w_up, w_down, fill_count, slot_index.T, expert_id.T, gate_weight.T)
        return pl.pallas_call(
            kernel,
            out_shape=pltpu.VMEM((tokens, width), bf16),
            in_specs=[pl.BlockSpec(memory_space=pl.ANY)] * len(operands),
            out_specs=pl.BlockSpec(memory_space=pltpu.VMEM),
            scratch_shapes=scratch,
            compiler_params=pltpu.CompilerParams(
                collective_id=0, has_side_effects=True, vmem_limit_bytes=44 * 1024 * 1024),
            name="expert_return",
        )(*(pltpu.with_memory_space_constraint(array, pltpu.HBM) for array in operands))

    token_spec = P(("dp", "ep"))
    in_specs = (P("dp", "ep"), P("ep"), P("ep"), P("ep"), P("dp", "ep"), token_spec, token_spec, token_spec)
    return jax.shard_map(local_step, mesh=mesh, in_specs=in_specs, out_specs=token_spec, check_vma=False)
```

```python
import jax
import jax.numpy as jnp
from jax import lax
from jax.experimental import pallas as pl
from jax.experimental.pallas import tpu as pltpu
from jax.sharding import PartitionSpec as P

MESH = pl.DeviceIdType.MESH
RING = 4
CHUNK = 256
DIRECT = 64
LENT = 32
BF16_MAX = 3.3895313892515355e38


def split3(value):
    high = jnp.minimum(value, BF16_MAX).astype(jnp.bfloat16)
    rest = value - high.astype(jnp.float32)
    middle = rest.astype(jnp.bfloat16)
    low = (rest - middle.astype(jnp.float32)).astype(jnp.bfloat16)
    return jnp.concatenate([high, middle, low], axis=0)


def kernel(x_hbm, wg_hbm, wu_hbm, wd_hbm, fill_hbm, slot_hbm, expert_hbm, gate_hbm, out_ref,
           x_buf, w_buf, wd_buf, fill_buf, id_buf, gate_buf,
           route_out, route_in, mix, hid, rows_buf, sums, from_peer, link_out, link_in, side_in, lent_in, lent_out,
           w_sem, x_sem, small_sem, send_sem, route_recv, give_recv, link_recv, side_recv, lent_recv):
    experts = wg_hbm.shape[0]
    capacity, width = x_hbm.shape[2:]
    choices, tokens = slot_hbm.shape
    chunks = width // CHUNK
    pair = 2 * capacity
    half = experts // 2
    group = lax.axis_index("dp")
    me = lax.axis_index("ep")
    core = lax.rem(me, 2)
    chip = me // 2
    partner = chip * 2 + (1 - core)
    far = (1 - chip) * 2 + core
    far_other = (1 - chip) * 2 + (1 - core)
    sources = (far_other, far, partner, me)

    def start_expert(e):
        for role in range(2):
            pltpu.make_async_copy(
                x_hbm.at[sources[role], e], x_buf.at[e, pl.ds(role * capacity, capacity)],
                x_sem.at[lax.rem(e, RING)]).start()
        for which, src in enumerate((wg_hbm, wu_hbm)):
            pltpu.make_async_copy(src.at[e], w_buf.at[e, which], w_sem.at[lax.rem(e, RING)]).start()

    def start_step(e, carry):
        start_expert(e)
        return carry

    def early_down_copy(e):
        return pltpu.make_async_copy(
            wd_hbm.at[e, :, pl.ds(0, CHUNK)], wd_buf.at[e, :, pl.ds(0, CHUNK)], x_sem.at[lax.rem(e + half, RING)])

    def wait_expert(e, late):
        part = x_buf.at[e] if late else x_buf.at[e, pl.ds(0, pair)]
        pltpu.make_async_copy(part, part, x_sem.at[lax.rem(e, RING)]).wait()
        pltpu.make_async_copy(w_buf.at[e], w_buf.at[e], w_sem.at[lax.rem(e, RING)]).wait()

    def down_copy(n):
        some = pl.ds(half, half) if n == 0 else pl.ds(0, experts)
        cols = pl.ds(n * CHUNK, CHUNK)
        return pltpu.make_async_copy(
            wd_hbm.at[some, :, cols], wd_buf.at[some, :, cols], w_sem.at[(experts + n) % RING])

    small = [pltpu.make_async_copy(src, dst, small_sem.at[i]) for i, (src, dst) in enumerate(
        ((slot_hbm, id_buf.at[0]), (expert_hbm, id_buf.at[1]), (gate_hbm, gate_buf), (fill_hbm, fill_buf)))]
    for copy in small:
        copy.start()
    lax.fori_loop(0, RING, start_step, 0)

    barrier = pltpu.get_barrier_semaphore()
    for peer in (partner, far, far_other):
        pl.semaphore_signal(barrier, inc=1, device_id=(group, peer), device_id_type=MESH)

    for copy in small:
        copy.wait()
    slot = id_buf[0]
    code = jnp.where(slot >= 0, id_buf[1] * capacity + slot, -1)
    route_out[0:choices] = code.astype(jnp.float32)
    route_out[choices:] = gate_buf[...]

    with jax.named_scope("bar"):
        pl.semaphore_wait(barrier, 3)
    for role, peer in ((0, far_other), (1, far), (2, partner)):
        pltpu.make_async_remote_copy(
            src_ref=route_out, dst_ref=route_in.at[role], send_sem=send_sem, recv_sem=route_recv,
            device_id=(group, peer), device_id_type=MESH).start()

    def route_all(src, dst):
        return pltpu.make_async_remote_copy(
            src_ref=route_in, dst_ref=route_in, send_sem=send_sem, recv_sem=route_recv,
            device_id=(group, partner), device_id_type=MESH)

    def hidden(first, e):
        rows = x_buf[e, pl.ds(first * capacity, pair)]
        pre_gate = jnp.dot(rows, w_buf[e, 0], preferred_element_type=jnp.float32)
        pre_up = jnp.dot(rows, w_buf[e, 1], preferred_element_type=jnp.float32)
        value = jax.nn.silu(pre_gate) * pre_up
        row = lax.broadcasted_iota(jnp.int32, value.shape, 0)
        limit = jnp.where(row < capacity, fill_buf[sources[first], e], fill_buf[sources[first + 1], e] + capacity)
        hid[e, pl.ds(first * capacity, pair)] = jnp.where(row < limit, value, 0.0).astype(jnp.bfloat16)

    def first_step(e, carry):
        with jax.named_scope("w_e"):
            wait_expert(e, False)

        @pl.when(e + RING >= half)
        def _():
            early_down_copy(e + RING - half).start()

        start_expert(e + RING)
        with jax.named_scope("hid"):
            hidden(0, e)
        return carry

    def late_step(e, carry):
        with jax.named_scope("w_e"):
            wait_expert(e, True)

        @pl.when(e + RING < experts)
        def _():
            early_down_copy(e + RING - half).start()
            start_expert(e + RING)

        for n in range(RING):
            @pl.when(e + RING == experts + n)
            def _():
                down_copy(n).start()

        with jax.named_scope("hid"):
            rows_of(0, 0, e - half)
            hidden(0, e)
        return carry

    def build_mix(role):
        route = route_out if role == 3 else route_in.at[role]
        code = route[0:choices].astype(jnp.int32)
        gate = route[choices:]
        row = lax.broadcasted_iota(jnp.int32, (experts * capacity, tokens), 0) + me * (experts * capacity)
        value = jnp.zeros((experts * capacity, tokens), jnp.float32)
        for j in range(choices):
            value = jnp.where(row == code[j:j + 1], gate[j:j + 1], value)
        value = value.T
        block = tokens // 2
        mix[role, 0:3 * block] = split3(value[:block])
        mix[role, 3 * block:] = split3(value[block:])

    def rows_of(first, n, e):
        value = jnp.dot(hid[e, pl.ds(first * capacity, pair)], wd_buf[e, :, pl.ds(n * CHUNK, CHUNK)],
                        preferred_element_type=jnp.float32).astype(jnp.bfloat16)
        here = pl.ds(e * capacity, capacity)
        rows_buf[0, here] = value[:capacity]
        rows_buf[1, here] = value[capacity:]

    def mixed(role):
        block = tokens // 2
        parts = []
        for part in range(2):
            value = jnp.dot(mix[role, pl.ds(part * 3 * block, 3 * block)], rows_buf[lax.rem(role, 2)],
                            preferred_element_type=jnp.float32)
            parts.append(value[:block] + value[block:2 * block] + value[2 * block:])
        return jnp.concatenate(parts, axis=0)

    def give_copy(kind, n):
        return pltpu.make_async_remote_copy(
            src_ref=sums.at[kind, 0, n], dst_ref=from_peer.at[kind, n], send_sem=send_sem,
            recv_sem=give_recv.at[n if kind == 0 else chunks], device_id=(group, partner), device_id_type=MESH)

    direct_copy = pltpu.make_async_remote_copy(
        src_ref=sums.at[0, 1 - core, 0, pl.ds(0, DIRECT)], dst_ref=side_in.at[pl.ds(core * DIRECT, DIRECT)],
        send_sem=send_sem, recv_sem=side_recv, device_id=(group, (1 - chip) * 2), device_id_type=MESH)
    rest_copy = pltpu.make_async_remote_copy(
        src_ref=link_out.at[0, pl.ds(0, DIRECT)], dst_ref=link_in.at[0, pl.ds(0, DIRECT)], send_sem=send_sem,
        recv_sem=side_recv, device_id=(group, far), device_id_type=MESH)
    lend_copy = pltpu.make_async_remote_copy(
        src_ref=sums.at[0, 1, 1, pl.ds(0, LENT)], dst_ref=lent_in, send_sem=send_sem, recv_sem=lent_recv,
        device_id=(group, partner), device_id_type=MESH)
    lent_copy = pltpu.make_async_remote_copy(
        src_ref=lent_out, dst_ref=side_in.at[pl.ds(2 * DIRECT, LENT)], send_sem=send_sem, recv_sem=side_recv,
        device_id=(group, far_other), device_id_type=MESH)
    own_copy = pltpu.make_async_remote_copy(
        src_ref=link_out.at[1, pl.ds(0, LENT)], dst_ref=link_in.at[1, pl.ds(0, LENT)], send_sem=send_sem,
        recv_sem=side_recv, device_id=(group, far), device_id_type=MESH)

    def link_copy(n):
        skip = DIRECT if n == 0 else LENT if n == 1 else 0
        part = pl.ds(skip, tokens - skip)
        return pltpu.make_async_remote_copy(
            src_ref=link_out.at[n, part], dst_ref=link_in.at[n, part], send_sem=send_sem,
            recv_sem=link_recv.at[n], device_id=(group, far), device_id_type=MESH)

    def send_on(n):
        give_copy(0, n).wait_recv()
        if n == 1:
            @pl.when(core == 1)
            def _():
                lend_copy.wait_recv()
                lent_out[...] = sums[0, 0, 1, 0:LENT] + lent_in[...]
                lent_copy.start()
        link_out[n] = sums[0, 1, n] + from_peer[0, n]
        if n <= 1:
            @pl.when(core == 1)
            def _():
                (rest_copy, own_copy)[n].start()
        link_copy(n).start()

    lax.fori_loop(0, half, first_step, 0)
    with jax.named_scope("w_route"):
        route_all(0, 0).wait_recv()
    with jax.named_scope("mix"):
        build_mix(0)
    lax.fori_loop(half, half + 2, late_step, 0)
    with jax.named_scope("mix"):
        build_mix(1)
    lax.fori_loop(half + 2, experts, late_step, 0)

    def remote_rows(n, between=lambda: None):
        with jax.named_scope("w_d"):
            down_copy(n).wait()
        if n + RING < chunks:
            down_copy(n + RING).start()
        with jax.named_scope("rows"):
            for e in range(half, experts):
                rows_of(0, n, e)
        between()
        if n > 0:
            with jax.named_scope("rows"):
                for e in range(half):
                    rows_of(0, n, e)

    def remote_sums(n):
        with jax.named_scope("mixed"):
            if n == 0:
                sums[0, 1 - core, 0] = mixed(1 - core)

                @pl.when(core == 1)
                def _():
                    give_copy(0, 0).start()

                direct_copy.start()
                sums[0, core, 0] = mixed(core)

                @pl.when(core == 0)
                def _():
                    give_copy(0, 0).start()
            else:
                sums[0, 0, n] = mixed(0)
                sums[0, 1, n] = mixed(1)
                give_copy(0, n).start()
            if n == 1:
                @pl.when(core == 0)
                def _():
                    lend_copy.start()

    remote_rows(0)
    for role in (2, 3):
        pltpu.make_async_copy(
            x_hbm.at[sources[role]], x_buf.at[:, pl.ds(role * capacity, capacity)], small_sem.at[0]).start()
    remote_sums(0)

    def send_first():
        @pl.when(core == 0)
        def _():
            with jax.named_scope("send_on"):
                send_on(0)

    remote_rows(1, send_first)
    remote_sums(1)

    @pl.when(core == 1)
    def _():
        with jax.named_scope("send_on"):
            send_on(0)

    for n in range(2, chunks):
        remote_rows(n)
        remote_sums(n)
        with jax.named_scope("send_on"):
            send_on(n - 1)

    local_rows = x_buf.at[:, pl.ds(pair, pair)]
    pltpu.make_async_copy(local_rows, local_rows, small_sem.at[0]).wait()

    def local_step(e, carry):
        hidden(2, e)
        return carry

    lax.fori_loop(0, 2, local_step, 0)
    send_on(chunks - 1)
    with jax.named_scope("phase1L"):
        lax.fori_loop(2, experts, local_step, 0)
    for role in (2, 3):
        build_mix(role)
    for n in range(chunks):
        with jax.named_scope("rows2"):
            for e in range(experts):
                rows_of(2, n, e)
        with jax.named_scope("mixed2"):
            sums[1, 0, n] = mixed(2)
            sums[1, 1, n] = mixed(3)
            give_copy(1, n).start()

    with jax.named_scope("fin_give"):
        pltpu.make_async_remote_copy(
            src_ref=sums.at[1, 0], dst_ref=from_peer.at[1], send_sem=send_sem, recv_sem=give_recv.at[chunks],
            device_id=(group, partner), device_id_type=MESH).wait_recv()

    with jax.named_scope("fin_side"):
        @pl.when(core == 0)
        def _():
            pltpu.make_async_remote_copy(
                src_ref=side_in, dst_ref=side_in, send_sem=send_sem, recv_sem=side_recv,
                device_id=(group, far), device_id_type=MESH).wait_recv()
            link_in[0, 0:DIRECT] = side_in[0:DIRECT] + side_in[DIRECT:2 * DIRECT]
            link_in[1, 0:LENT] = side_in[2 * DIRECT:]

        @pl.when(core == 1)
        def _():
            both = link_in.at[0, pl.ds(0, DIRECT + LENT)]
            pltpu.make_async_remote_copy(
                src_ref=both, dst_ref=both, send_sem=send_sem, recv_sem=side_recv,
                device_id=(group, far), device_id_type=MESH).wait_recv()

    for n in range(chunks):
        near = sums[1, 1, n] + from_peer[1, n]
        with jax.named_scope("fin_link"):
            link_copy(n).wait_recv()
        out_ref[:, pl.ds(n * CHUNK, CHUNK)] = (near + link_in[n]).astype(jnp.bfloat16)

    with jax.named_scope("w_send"):
        def wait_sent(ref):
            pltpu.make_async_remote_copy(
                src_ref=ref, dst_ref=ref, send_sem=send_sem, recv_sem=side_recv,
                device_id=(group, far), device_id_type=MESH).wait_send()

        wait_sent(route_in)
        wait_sent(from_peer)
        for n in range(chunks):
            link_copy(n).wait_send()
        direct_copy.wait_send()

        @pl.when(core == 0)
        def _():
            lend_copy.wait_send()

        @pl.when(core == 1)
        def _():
            for copy in (rest_copy, own_copy, lent_copy):
                copy.wait_send()


def solution(mesh):
    def local_step(dispatched, w_gate, w_up, w_down, fill_count, slot_index, expert_id, gate_weight):
        sources, experts, capacity, width = dispatched.shape
        ffn = w_gate.shape[2]
        tokens, choices = slot_index.shape
        chunks = width // CHUNK
        f32, bf16 = jnp.float32, jnp.bfloat16
        scratch = [
            pltpu.VMEM((experts, sources * capacity, width), bf16),
            pltpu.VMEM((experts, 2, width, ffn), bf16),
            pltpu.VMEM((experts, ffn, width), bf16),
            pltpu.SMEM((sources, experts), jnp.int32),
            pltpu.VMEM((2, choices, tokens), jnp.int32),
            pltpu.VMEM((choices, tokens), f32),
            pltpu.VMEM((2 * choices, tokens), f32),
            pltpu.VMEM((3, 2 * choices, tokens), f32),
            pltpu.VMEM((4, 3 * tokens, experts * capacity), bf16),
            pltpu.VMEM((experts, sources * capacity, ffn), bf16),
            pltpu.VMEM((2, experts * capacity, CHUNK), bf16),
            pltpu.VMEM((2, 2, chunks, tokens, CHUNK), f32),
            pltpu.VMEM((2, chunks, tokens, CHUNK), f32),
            pltpu.VMEM((chunks, tokens, CHUNK), f32),
            pltpu.VMEM((chunks, tokens, CHUNK), f32),
            pltpu.VMEM((2 * DIRECT + LENT, CHUNK), f32),
            pltpu.VMEM((LENT, CHUNK), f32),
            pltpu.VMEM((LENT, CHUNK), f32),
            pltpu.SemaphoreType.DMA((RING,)),
            pltpu.SemaphoreType.DMA((RING,)),
            pltpu.SemaphoreType.DMA((4,)),
            pltpu.SemaphoreType.DMA,
            pltpu.SemaphoreType.DMA,
            pltpu.SemaphoreType.DMA((chunks + 1,)),
            pltpu.SemaphoreType.DMA((chunks,)),
            pltpu.SemaphoreType.DMA,
            pltpu.SemaphoreType.DMA,
        ]
        operands = (dispatched, w_gate, w_up, w_down, fill_count, slot_index.T, expert_id.T, gate_weight.T)
        return pl.pallas_call(
            kernel,
            out_shape=pltpu.VMEM((tokens, width), bf16),
            in_specs=[pl.BlockSpec(memory_space=pl.ANY)] * len(operands),
            out_specs=pl.BlockSpec(memory_space=pltpu.VMEM),
            scratch_shapes=scratch,
            compiler_params=pltpu.CompilerParams(
                collective_id=0, has_side_effects=True, vmem_limit_bytes=44 * 1024 * 1024),
            name="expert_return",
        )(*(pltpu.with_memory_space_constraint(array, pltpu.HBM) for array in operands))

    token_spec = P(("dp", "ep"))
    in_specs = (P("dp", "ep"), P("ep"), P("ep"), P("ep"), P("dp", "ep"), token_spec, token_spec, token_spec)
    return jax.shard_map(local_step, mesh=mesh, in_specs=in_specs, out_specs=token_spec, check_vma=False)
```

```python
import jax
import jax.numpy as jnp
from jax import lax
from jax.experimental import pallas as pl
from jax.experimental.pallas import tpu as pltpu
from jax.sharding import PartitionSpec as P

MESH = pl.DeviceIdType.MESH
CHUNK = 256
EARLY = 3
DIRECT = 64
LENT = 32
BF16_MAX = 3.3895313892515355e38


def split3(value):
    high = jnp.minimum(value, BF16_MAX).astype(jnp.bfloat16)
    rest = value - high.astype(jnp.float32)
    middle = rest.astype(jnp.bfloat16)
    low = (rest - middle.astype(jnp.float32)).astype(jnp.bfloat16)
    return jnp.concatenate([high, middle, low], axis=0)


def kernel(x_hbm, wg_hbm, wu_hbm, wd_hbm, fill_hbm, slot_hbm, expert_hbm, gate_hbm, out_ref,
           x_buf, w_buf, wd_buf, fill_buf, id_buf, gate_buf,
           route_out, route_in, mix, hid, rows_buf, sums, from_peer, link_out, link_in, side_in, lent_in, lent_out,
           stream_sem, small_sem, send_sem, route_recv, give_recv, link_recv, side_recv, lent_recv):
    experts, _, ffn = wg_hbm.shape
    capacity, width = x_hbm.shape[2:]
    choices, tokens = slot_hbm.shape
    chunks = width // CHUNK
    pair = 2 * capacity
    half = experts // 2
    mid = experts - 1 - EARLY
    group = lax.axis_index("dp")
    me = lax.axis_index("ep")
    core = lax.rem(me, 2)
    chip = me // 2
    partner = chip * 2 + (1 - core)
    far = (1 - chip) * 2 + core
    far_other = (1 - chip) * 2 + (1 - core)
    sources = (far_other, far, partner, me)

    def start_expert(e, carry):
        for which, src in enumerate((wg_hbm, wu_hbm)):
            pltpu.make_async_copy(src.at[e], w_buf.at[e, which], stream_sem.at[e]).start()
        return carry

    def start_late_expert(e, carry):
        cols = pl.ds(0, CHUNK)
        pltpu.make_async_copy(wd_hbm.at[e - mid, :, cols], wd_buf.at[e - mid, :, cols], stream_sem.at[e]).start()
        return start_expert(e, carry)

    def wait_expert(e, late):
        values = 2 * width * ffn + (ffn * CHUNK if late else 0)
        part = x_buf.at[:, pl.ds(0, values // (experts * width))]
        pltpu.make_async_copy(part, part, stream_sem.at[e]).wait()

    def down_copy(n):
        some = pl.ds(EARLY, experts - EARLY) if n == 0 else pl.ds(0, experts)
        cols = pl.ds(n * CHUNK, CHUNK)
        return pltpu.make_async_copy(wd_hbm.at[some, :, cols], wd_buf.at[some, :, cols], stream_sem.at[n])

    def start_first_chunk():
        cols = pl.ds(0, CHUNK)
        for e in range(EARLY, experts):
            pltpu.make_async_copy(wd_hbm.at[e, :, cols], wd_buf.at[e, :, cols], stream_sem.at[0]).start()

    small = [pltpu.make_async_copy(src, dst, small_sem.at[i]) for i, src, dst in (
        (0, slot_hbm, id_buf.at[0]), (0, expert_hbm, id_buf.at[1]), (1, gate_hbm, gate_buf), (2, fill_hbm, fill_buf))]
    for copy in small:
        copy.start()
    def start_rows(first, count, sem):
        for role in (first, first + 1):
            some = pl.ds(0, count) if count < experts else pl.ds(0, experts)
            pltpu.make_async_copy(
                x_hbm.at[sources[role], some], x_buf.at[some, pl.ds(role * capacity, capacity)], sem).start()

    start_rows(0, experts, small_sem.at[3])
    lax.fori_loop(0, half, start_expert, 0)

    barrier = pltpu.get_barrier_semaphore()
    for peer in (partner, far, far_other):
        pl.semaphore_signal(barrier, inc=1, device_id=(group, peer), device_id_type=MESH)

    lax.fori_loop(half, mid, start_expert, 0)
    lax.fori_loop(mid, experts - 1, start_late_expert, 0)
    start_expert(experts - 1, 0)

    pltpu.make_async_copy(id_buf, id_buf, small_sem.at[0]).wait()
    for copy in small[2:]:
        copy.wait()
    slot = id_buf[0]
    code = jnp.where(slot >= 0, id_buf[1] * capacity + slot, -1)
    route_out[0:choices] = code.astype(jnp.float32)
    route_out[choices:] = gate_buf[...]

    with jax.named_scope("bar"):
        pl.semaphore_wait(barrier, 3)
    for role, peer in ((0, far_other), (1, far), (2, partner)):
        pltpu.make_async_remote_copy(
            src_ref=route_out, dst_ref=route_in.at[role], send_sem=send_sem, recv_sem=route_recv,
            device_id=(group, peer), device_id_type=MESH).start()

    def route_all(src, dst):
        return pltpu.make_async_remote_copy(
            src_ref=route_in, dst_ref=route_in, send_sem=send_sem, recv_sem=route_recv,
            device_id=(group, partner), device_id_type=MESH)

    def hidden(first, e):
        rows = x_buf[e, pl.ds(first * capacity, pair)]
        pre_gate = jnp.dot(rows, w_buf[e, 0], preferred_element_type=jnp.float32)
        pre_up = jnp.dot(rows, w_buf[e, 1], preferred_element_type=jnp.float32)
        value = jax.nn.silu(pre_gate) * pre_up
        row = lax.broadcasted_iota(jnp.int32, value.shape, 0)
        limit = jnp.where(row < capacity, fill_buf[sources[first], e], fill_buf[sources[first + 1], e] + capacity)
        hid[e, pl.ds(first * capacity, pair)] = jnp.where(row < limit, value, 0.0).astype(jnp.bfloat16)

    def first_step(e, carry):
        with jax.named_scope("w_e"):
            wait_expert(e, False)
        @pl.when(e == 0)
        def _():
            start_first_chunk()

        with jax.named_scope("hid"):
            hidden(0, e)
        return carry

    def late_step(e, carry):
        with jax.named_scope("w_e"):
            wait_expert(e, True)
        with jax.named_scope("hid"):
            rows_of(0, 0, e - mid)
            hidden(0, e)
        return carry

    def build_mix(role):
        route = route_out if role == 3 else route_in.at[role]
        code = route[0:choices].astype(jnp.int32)
        gate = route[choices:]
        row = lax.broadcasted_iota(jnp.int32, (experts * capacity, tokens), 0) + me * (experts * capacity)
        value = jnp.zeros((experts * capacity, tokens), jnp.float32)
        for j in range(choices):
            value = jnp.where(row == code[j:j + 1], gate[j:j + 1], value)
        value = value.T
        block = tokens // 2
        mix[role, 0:3 * block] = split3(value[:block])
        mix[role, 3 * block:] = split3(value[block:])

    def rows_of(first, n, e):
        value = jnp.dot(hid[e, pl.ds(first * capacity, pair)], wd_buf[e, :, pl.ds(n * CHUNK, CHUNK)],
                        preferred_element_type=jnp.float32).astype(jnp.bfloat16)
        here = pl.ds(e * capacity, capacity)
        rows_buf[0, here] = value[:capacity]
        rows_buf[1, here] = value[capacity:]

    def mixed(role):
        block = tokens // 2
        parts = []
        for part in range(2):
            value = jnp.dot(mix[role, pl.ds(part * 3 * block, 3 * block)], rows_buf[lax.rem(role, 2)],
                            preferred_element_type=jnp.float32)
            parts.append(value[:block] + value[block:2 * block] + value[2 * block:])
        return jnp.concatenate(parts, axis=0)

    def give_copy(kind, n):
        return pltpu.make_async_remote_copy(
            src_ref=sums.at[kind, 0, n], dst_ref=from_peer.at[kind, n], send_sem=send_sem,
            recv_sem=give_recv.at[n if kind == 0 else chunks], device_id=(group, partner), device_id_type=MESH)

    direct_copy = pltpu.make_async_remote_copy(
        src_ref=sums.at[0, 1 - core, 0, pl.ds(0, DIRECT)], dst_ref=side_in.at[pl.ds(core * DIRECT, DIRECT)],
        send_sem=send_sem, recv_sem=side_recv, device_id=(group, (1 - chip) * 2), device_id_type=MESH)
    rest_copy = pltpu.make_async_remote_copy(
        src_ref=link_out.at[0, pl.ds(0, DIRECT)], dst_ref=link_in.at[0, pl.ds(0, DIRECT)], send_sem=send_sem,
        recv_sem=side_recv, device_id=(group, far), device_id_type=MESH)
    lend_copy = pltpu.make_async_remote_copy(
        src_ref=sums.at[0, 1, 1, pl.ds(0, LENT)], dst_ref=lent_in, send_sem=send_sem, recv_sem=lent_recv,
        device_id=(group, partner), device_id_type=MESH)
    lent_copy = pltpu.make_async_remote_copy(
        src_ref=lent_out, dst_ref=side_in.at[pl.ds(2 * DIRECT, LENT)], send_sem=send_sem, recv_sem=side_recv,
        device_id=(group, far_other), device_id_type=MESH)
    own_copy = pltpu.make_async_remote_copy(
        src_ref=link_out.at[1, pl.ds(0, LENT)], dst_ref=link_in.at[1, pl.ds(0, LENT)], send_sem=send_sem,
        recv_sem=side_recv, device_id=(group, far), device_id_type=MESH)

    def link_copy(n):
        skip = DIRECT if n == 0 else LENT if n == 1 else 0
        part = pl.ds(skip, tokens - skip)
        return pltpu.make_async_remote_copy(
            src_ref=link_out.at[n, part], dst_ref=link_in.at[n, part], send_sem=send_sem,
            recv_sem=link_recv.at[n // (chunks - 1)], device_id=(group, far), device_id_type=MESH)

    def send_on(n):
        give_copy(0, n).wait_recv()
        if n == 1:
            @pl.when(core == 1)
            def _():
                lend_copy.wait_recv()
                lent_out[...] = sums[0, 0, 1, 0:LENT] + lent_in[...]
                lent_copy.start()
        link_out[n] = sums[0, 1, n] + from_peer[0, n]
        if n <= 1:
            @pl.when(core == 1)
            def _():
                (rest_copy, own_copy)[n].start()
        link_copy(n).start()

    remote_rows_in = x_buf.at[:, pl.ds(0, pair)]
    pltpu.make_async_copy(remote_rows_in, remote_rows_in, small_sem.at[3]).wait()
    lax.fori_loop(0, half, first_step, 0)
    with jax.named_scope("w_route"):
        route_all(0, 0).wait_recv()
    with jax.named_scope("mix"):
        build_mix(0)
    lax.fori_loop(half, mid, first_step, 0)
    with jax.named_scope("mix"):
        build_mix(1)
    lax.fori_loop(mid, experts - 1, late_step, 0)
    down_copy(1).start()
    lax.fori_loop(experts - 1, experts, first_step, 0)
    for n in range(2, chunks):
        down_copy(n).start()

    def remote_rows(n, between=lambda: None):
        with jax.named_scope("w_d"):
            down_copy(n).wait()
        with jax.named_scope("rows"):
            for e in range(EARLY, experts) if n == 0 else range(half):
                rows_of(0, n, e)
        between()
        if n > 0:
            with jax.named_scope("rows"):
                for e in range(half, experts):
                    rows_of(0, n, e)

    def remote_sums(n):
        with jax.named_scope("mixed"):
            if n == 0:
                sums[0, 1 - core, 0] = mixed(1 - core)

                @pl.when(core == 1)
                def _():
                    give_copy(0, 0).start()

                direct_copy.start()
                sums[0, core, 0] = mixed(core)

                @pl.when(core == 0)
                def _():
                    give_copy(0, 0).start()
            else:
                sums[0, 0, n] = mixed(0)
                sums[0, 1, n] = mixed(1)
                give_copy(0, n).start()
            if n == 1:
                @pl.when(core == 0)
                def _():
                    lend_copy.start()

    remote_rows(0)
    for role in (2, 3):
        pltpu.make_async_copy(
            x_hbm.at[sources[role]], x_buf.at[:, pl.ds(role * capacity, capacity)], stream_sem.at[half]).start()
    remote_sums(0)

    def send_first():
        @pl.when(core == 0)
        def _():
            with jax.named_scope("send_on"):
                send_on(0)

    remote_rows(1, send_first)
    remote_sums(1)

    @pl.when(core == 1)
    def _():
        with jax.named_scope("send_on"):
            send_on(0)

    for n in range(2, chunks):
        remote_rows(n)
        remote_sums(n)
        with jax.named_scope("send_on"):
            send_on(n - 1)

    local_rows = x_buf.at[:, pl.ds(pair, pair)]
    pltpu.make_async_copy(local_rows, local_rows, stream_sem.at[half]).wait()

    def local_step(e, carry):
        hidden(2, e)
        return carry

    lax.fori_loop(0, 2, local_step, 0)
    send_on(chunks - 1)
    with jax.named_scope("phase1L"):
        lax.fori_loop(2, experts, local_step, 0)
    for role in (2, 3):
        build_mix(role)
    for n in range(chunks):
        with jax.named_scope("rows2"):
            for e in range(experts):
                rows_of(2, n, e)
        with jax.named_scope("mixed2"):
            sums[1, 0, n] = mixed(2)
            sums[1, 1, n] = mixed(3)
            give_copy(1, n).start()

    with jax.named_scope("fin_give"):
        pltpu.make_async_remote_copy(
            src_ref=sums.at[1, 0], dst_ref=from_peer.at[1], send_sem=send_sem, recv_sem=give_recv.at[chunks],
            device_id=(group, partner), device_id_type=MESH).wait_recv()

    with jax.named_scope("fin_side"):
        @pl.when(core == 0)
        def _():
            pltpu.make_async_remote_copy(
                src_ref=side_in, dst_ref=side_in, send_sem=send_sem, recv_sem=side_recv,
                device_id=(group, far), device_id_type=MESH).wait_recv()
            link_in[0, 0:DIRECT] = side_in[0:DIRECT] + side_in[DIRECT:2 * DIRECT]
            link_in[1, 0:LENT] = side_in[2 * DIRECT:]

        @pl.when(core == 1)
        def _():
            both = link_in.at[0, pl.ds(0, DIRECT + LENT)]
            pltpu.make_async_remote_copy(
                src_ref=both, dst_ref=both, send_sem=send_sem, recv_sem=side_recv,
                device_id=(group, far), device_id_type=MESH).wait_recv()

    for n in range(chunks):
        near = sums[1, 1, n] + from_peer[1, n]
        with jax.named_scope("fin_link"):
            if n == 0:
                count = ((chunks - 1) * tokens - DIRECT - LENT) // chunks
                part = link_in.at[:, pl.ds(0, count)]
                pltpu.make_async_remote_copy(
                    src_ref=part, dst_ref=part, send_sem=send_sem, recv_sem=link_recv.at[0],
                    device_id=(group, far), device_id_type=MESH).wait_recv()
            if n == chunks - 1:
                link_copy(n).wait_recv()
        out_ref[:, pl.ds(n * CHUNK, CHUNK)] = (near + link_in[n]).astype(jnp.bfloat16)

    with jax.named_scope("w_send"):
        def wait_sent(ref):
            pltpu.make_async_remote_copy(
                src_ref=ref, dst_ref=ref, send_sem=send_sem, recv_sem=side_recv,
                device_id=(group, far), device_id_type=MESH).wait_send()

        wait_sent(route_in)
        wait_sent(from_peer)
        for n in range(chunks):
            link_copy(n).wait_send()
        direct_copy.wait_send()

        @pl.when(core == 0)
        def _():
            lend_copy.wait_send()

        @pl.when(core == 1)
        def _():
            for copy in (rest_copy, own_copy, lent_copy):
                copy.wait_send()


def solution(mesh):
    def local_step(dispatched, w_gate, w_up, w_down, fill_count, slot_index, expert_id, gate_weight):
        sources, experts, capacity, width = dispatched.shape
        ffn = w_gate.shape[2]
        tokens, choices = slot_index.shape
        chunks = width // CHUNK
        f32, bf16 = jnp.float32, jnp.bfloat16
        scratch = [
            pltpu.VMEM((experts, sources * capacity, width), bf16),
            pltpu.VMEM((experts, 2, width, ffn), bf16),
            pltpu.VMEM((experts, ffn, width), bf16),
            pltpu.SMEM((sources, experts), jnp.int32),
            pltpu.VMEM((2, choices, tokens), jnp.int32),
            pltpu.VMEM((choices, tokens), f32),
            pltpu.VMEM((2 * choices, tokens), f32),
            pltpu.VMEM((3, 2 * choices, tokens), f32),
            pltpu.VMEM((4, 3 * tokens, experts * capacity), bf16),
            pltpu.VMEM((experts, sources * capacity, ffn), bf16),
            pltpu.VMEM((2, experts * capacity, CHUNK), bf16),
            pltpu.VMEM((2, 2, chunks, tokens, CHUNK), f32),
            pltpu.VMEM((2, chunks, tokens, CHUNK), f32),
            pltpu.VMEM((chunks, tokens, CHUNK), f32),
            pltpu.VMEM((chunks, tokens, CHUNK), f32),
            pltpu.VMEM((2 * DIRECT + LENT, CHUNK), f32),
            pltpu.VMEM((LENT, CHUNK), f32),
            pltpu.VMEM((LENT, CHUNK), f32),
            pltpu.SemaphoreType.DMA((experts,)),
            pltpu.SemaphoreType.DMA((4,)),
            pltpu.SemaphoreType.DMA,
            pltpu.SemaphoreType.DMA,
            pltpu.SemaphoreType.DMA((chunks + 1,)),
            pltpu.SemaphoreType.DMA((2,)),
            pltpu.SemaphoreType.DMA,
            pltpu.SemaphoreType.DMA,
        ]
        operands = (dispatched, w_gate, w_up, w_down, fill_count, slot_index.T, expert_id.T, gate_weight.T)
        return pl.pallas_call(
            kernel,
            out_shape=pltpu.VMEM((tokens, width), bf16),
            in_specs=[pl.BlockSpec(memory_space=pl.ANY)] * len(operands),
            out_specs=pl.BlockSpec(memory_space=pltpu.VMEM),
            scratch_shapes=scratch,
            compiler_params=pltpu.CompilerParams(
                collective_id=0, has_side_effects=True, vmem_limit_bytes=44 * 1024 * 1024),
            name="expert_return",
        )(*(pltpu.with_memory_space_constraint(array, pltpu.HBM) for array in operands))

    token_spec = P(("dp", "ep"))
    in_specs = (P("dp", "ep"), P("ep"), P("ep"), P("ep"), P("dp", "ep"), token_spec, token_spec, token_spec)
    return jax.shard_map(local_step, mesh=mesh, in_specs=in_specs, out_specs=token_spec, check_vma=False)
```

```python
import jax
import jax.numpy as jnp
from jax import lax
from jax.experimental import pallas as pl
from jax.experimental.pallas import tpu as pltpu
from jax.sharding import PartitionSpec as P

MESH = pl.DeviceIdType.MESH
CHUNK = 256
EARLY = 3
DIRECT = 64
LENT = 64
AWAY = 80
BF16_MAX = 3.3895313892515355e38


def split3(value):
    high = jnp.minimum(value, BF16_MAX).astype(jnp.bfloat16)
    rest = value - high.astype(jnp.float32)
    middle = rest.astype(jnp.bfloat16)
    low = (rest - middle.astype(jnp.float32)).astype(jnp.bfloat16)
    return jnp.concatenate([high, middle, low], axis=0)


def kernel(x_hbm, wg_hbm, wu_hbm, wd_hbm, fill_hbm, slot_hbm, expert_hbm, gate_hbm, out_ref,
           x_buf, w_buf, wd_buf, fill_buf, id_buf, gate_buf,
           route_out, route_in, mix, hid, rows_buf, sums, from_peer, link_out, link_in, side_in, lent_in, lent_out,
           away_out, away_in, final_out, final_in,
           stream_sem, small_sem, send_sem, route_recv, give_recv, link_recv, side_recv, lent_recv,
           away_recv):
    experts, _, ffn = wg_hbm.shape
    capacity, width = x_hbm.shape[2:]
    choices, tokens = slot_hbm.shape
    chunks = width // CHUNK
    pair = 2 * capacity
    half = experts // 2
    mid = experts - 1 - EARLY
    group = lax.axis_index("dp")
    me = lax.axis_index("ep")
    core = lax.rem(me, 2)
    chip = me // 2
    partner = chip * 2 + (1 - core)
    far = (1 - chip) * 2 + core
    far_other = (1 - chip) * 2 + (1 - core)
    sources = (far_other, far, partner, me)

    def start_expert(e, carry):
        for which, src in enumerate((wg_hbm, wu_hbm)):
            pltpu.make_async_copy(src.at[e], w_buf.at[e, which], stream_sem.at[e]).start()
        return carry

    def start_late_expert(e, carry):
        cols = pl.ds(0, CHUNK)
        pltpu.make_async_copy(wd_hbm.at[e - mid, :, cols], wd_buf.at[e - mid, :, cols], stream_sem.at[e]).start()
        return start_expert(e, carry)

    def wait_expert(e, late):
        values = 2 * width * ffn + (ffn * CHUNK if late else 0)
        part = x_buf.at[:, pl.ds(0, values // (experts * width))]
        pltpu.make_async_copy(part, part, stream_sem.at[e]).wait()

    def down_copy(n):
        some = pl.ds(EARLY, experts - EARLY) if n == 0 else pl.ds(0, experts)
        cols = pl.ds(n * CHUNK, CHUNK)
        return pltpu.make_async_copy(wd_hbm.at[some, :, cols], wd_buf.at[some, :, cols], stream_sem.at[n])

    def start_first_chunk():
        cols = pl.ds(0, CHUNK)
        for e in range(EARLY, experts):
            pltpu.make_async_copy(wd_hbm.at[e, :, cols], wd_buf.at[e, :, cols], stream_sem.at[0]).start()

    small = [pltpu.make_async_copy(src, dst, small_sem.at[i]) for i, src, dst in (
        (0, slot_hbm, id_buf.at[0]), (0, expert_hbm, id_buf.at[1]), (1, gate_hbm, gate_buf), (2, fill_hbm, fill_buf))]
    for copy in small:
        copy.start()
    def start_rows(first, count, sem):
        for role in (first, first + 1):
            some = pl.ds(0, count) if count < experts else pl.ds(0, experts)
            pltpu.make_async_copy(
                x_hbm.at[sources[role], some], x_buf.at[some, pl.ds(role * capacity, capacity)], sem).start()

    start_rows(0, experts, small_sem.at[3])
    lax.fori_loop(0, half, start_expert, 0)

    barrier = pltpu.get_barrier_semaphore()
    for peer in (partner, far, far_other):
        pl.semaphore_signal(barrier, inc=1, device_id=(group, peer), device_id_type=MESH)

    lax.fori_loop(half, mid, start_expert, 0)
    lax.fori_loop(mid, experts - 1, start_late_expert, 0)
    start_expert(experts - 1, 0)

    pltpu.make_async_copy(id_buf, id_buf, small_sem.at[0]).wait()
    for copy in small[2:]:
        copy.wait()
    slot = id_buf[0]
    code = jnp.where(slot >= 0, id_buf[1] * capacity + slot, -1)
    route_out[0:choices] = code.astype(jnp.float32)
    route_out[choices:] = gate_buf[...]

    with jax.named_scope("bar"):
        pl.semaphore_wait(barrier, 3)
    for role, peer in ((0, far_other), (1, far), (2, partner)):
        pltpu.make_async_remote_copy(
            src_ref=route_out, dst_ref=route_in.at[role], send_sem=send_sem, recv_sem=route_recv,
            device_id=(group, peer), device_id_type=MESH).start()

    def route_all(src, dst):
        return pltpu.make_async_remote_copy(
            src_ref=route_in, dst_ref=route_in, send_sem=send_sem, recv_sem=route_recv,
            device_id=(group, partner), device_id_type=MESH)

    def hidden(first, e):
        rows = x_buf[e, pl.ds(first * capacity, pair)]
        pre_gate = jnp.dot(rows, w_buf[e, 0], preferred_element_type=jnp.float32)
        pre_up = jnp.dot(rows, w_buf[e, 1], preferred_element_type=jnp.float32)
        value = jax.nn.silu(pre_gate) * pre_up
        row = lax.broadcasted_iota(jnp.int32, value.shape, 0)
        limit = jnp.where(row < capacity, fill_buf[sources[first], e], fill_buf[sources[first + 1], e] + capacity)
        hid[e, pl.ds(first * capacity, pair)] = jnp.where(row < limit, value, 0.0).astype(jnp.bfloat16)

    def first_step(e, carry):
        with jax.named_scope("w_e"):
            wait_expert(e, False)
        @pl.when(e == 0)
        def _():
            start_first_chunk()

        with jax.named_scope("hid"):
            hidden(0, e)
        return carry

    def late_step(e, carry):
        with jax.named_scope("w_e"):
            wait_expert(e, True)
        with jax.named_scope("hid"):
            rows_of(0, 0, e - mid)
            hidden(0, e)
        return carry

    def build_mix(role):
        route = route_out if role == 3 else route_in.at[role]
        code = route[0:choices].astype(jnp.int32)
        gate = route[choices:]
        row = lax.broadcasted_iota(jnp.int32, (experts * capacity, tokens), 0) + me * (experts * capacity)
        value = jnp.zeros((experts * capacity, tokens), jnp.float32)
        for j in range(choices):
            value = jnp.where(row == code[j:j + 1], gate[j:j + 1], value)
        value = value.T
        block = tokens // 2
        mix[role, 0:3 * block] = split3(value[:block])
        mix[role, 3 * block:] = split3(value[block:])

    def rows_of(first, n, e):
        value = jnp.dot(hid[e, pl.ds(first * capacity, pair)], wd_buf[e, :, pl.ds(n * CHUNK, CHUNK)],
                        preferred_element_type=jnp.float32).astype(jnp.bfloat16)
        here = pl.ds(e * capacity, capacity)
        rows_buf[0, here] = value[:capacity]
        rows_buf[1, here] = value[capacity:]

    def mixed(role):
        block = tokens // 2
        parts = []
        for part in range(2):
            value = jnp.dot(mix[role, pl.ds(part * 3 * block, 3 * block)], rows_buf[lax.rem(role, 2)],
                            preferred_element_type=jnp.float32)
            parts.append(value[:block] + value[block:2 * block] + value[2 * block:])
        return jnp.concatenate(parts, axis=0)

    def give_copy(kind, n):
        return pltpu.make_async_remote_copy(
            src_ref=sums.at[kind, 0, n], dst_ref=from_peer.at[kind, n], send_sem=send_sem,
            recv_sem=give_recv.at[n if kind == 0 else chunks + (n == chunks - 1)], device_id=(group, partner), device_id_type=MESH)

    direct_copy = pltpu.make_async_remote_copy(
        src_ref=sums.at[0, 1 - core, 0, pl.ds(0, DIRECT)], dst_ref=side_in.at[pl.ds(core * DIRECT, DIRECT)],
        send_sem=send_sem, recv_sem=side_recv, device_id=(group, (1 - chip) * 2), device_id_type=MESH)
    rest_copy = pltpu.make_async_remote_copy(
        src_ref=link_out.at[0, pl.ds(0, DIRECT)], dst_ref=link_in.at[0, pl.ds(0, DIRECT)], send_sem=send_sem,
        recv_sem=side_recv, device_id=(group, far), device_id_type=MESH)
    lend_copy = pltpu.make_async_remote_copy(
        src_ref=sums.at[0, 1, 1, pl.ds(0, LENT)], dst_ref=lent_in, send_sem=send_sem, recv_sem=lent_recv,
        device_id=(group, partner), device_id_type=MESH)
    lent_copy = pltpu.make_async_remote_copy(
        src_ref=lent_out, dst_ref=side_in.at[pl.ds(2 * DIRECT, LENT)], send_sem=send_sem, recv_sem=side_recv,
        device_id=(group, far_other), device_id_type=MESH)
    own_copy = pltpu.make_async_remote_copy(
        src_ref=link_out.at[1, pl.ds(0, LENT)], dst_ref=link_in.at[1, pl.ds(0, LENT)], send_sem=send_sem,
        recv_sem=side_recv, device_id=(group, far), device_id_type=MESH)

    lends_last = (chip == 0) & (core == 1)
    adds_last = (chip == 1) & (core == 1)
    away_copy = pltpu.make_async_remote_copy(
        src_ref=away_out, dst_ref=away_in, send_sem=send_sem, recv_sem=away_recv,
        device_id=(group, far), device_id_type=MESH)
    final_copy = pltpu.make_async_remote_copy(
        src_ref=final_out, dst_ref=final_in, send_sem=send_sem, recv_sem=away_recv,
        device_id=(group, far), device_id_type=MESH)

    def last_copy(skip):
        part = pl.ds(skip, tokens - skip)
        n = chunks - 1
        return pltpu.make_async_remote_copy(
            src_ref=link_out.at[n, part], dst_ref=link_in.at[n, part], send_sem=send_sem,
            recv_sem=link_recv.at[1], device_id=(group, far), device_id_type=MESH)

    def link_copy(n):
        skip = DIRECT if n == 0 else LENT if n == 1 else 0
        part = pl.ds(skip, tokens - skip)
        return pltpu.make_async_remote_copy(
            src_ref=link_out.at[n, part], dst_ref=link_in.at[n, part], send_sem=send_sem,
            recv_sem=link_recv.at[0], device_id=(group, far), device_id_type=MESH)

    def send_on(n):
        give_copy(0, n).wait_recv()
        if n == 1:
            @pl.when(core == 1)
            def _():
                lend_copy.wait_recv()
                lent_out[...] = sums[0, 0, 1, 0:LENT] + lent_in[...]
                lent_copy.start()
        link_out[n] = sums[0, 1, n] + from_peer[0, n]
        if n <= 1:
            @pl.when(core == 1)
            def _():
                (rest_copy, own_copy)[n].start()
        if n < chunks - 1:
            link_copy(n).start()
        else:
            @pl.when(adds_last)
            def _():
                last_copy(AWAY).start()

            @pl.when(jnp.logical_not(adds_last))
            def _():
                last_copy(0).start()

    remote_rows_in = x_buf.at[:, pl.ds(0, pair)]
    pltpu.make_async_copy(remote_rows_in, remote_rows_in, small_sem.at[3]).wait()
    lax.fori_loop(0, half, first_step, 0)
    with jax.named_scope("w_route"):
        route_all(0, 0).wait_recv()
    with jax.named_scope("mix"):
        build_mix(0)
    lax.fori_loop(half, mid, first_step, 0)
    with jax.named_scope("mix"):
        build_mix(1)
    lax.fori_loop(mid, experts - 1, late_step, 0)
    down_copy(1).start()
    lax.fori_loop(experts - 1, experts, first_step, 0)
    for n in range(2, chunks):
        down_copy(n).start()

    def remote_rows(n, between=lambda: None):
        if n < chunks - 1:
            with jax.named_scope("w_d"):
                down_copy(n).wait()
        with jax.named_scope("rows"):
            for e in range(EARLY, experts) if n == 0 else range(half):
                rows_of(0, n, e)
        between()
        if n > 0:
            with jax.named_scope("rows"):
                for e in range(half, experts):
                    rows_of(0, n, e)

    def remote_sums(n):
        with jax.named_scope("mixed"):
            if n == 0:
                sums[0, 1 - core, 0] = mixed(1 - core)

                @pl.when(core == 1)
                def _():
                    give_copy(0, 0).start()

                direct_copy.start()
                sums[0, core, 0] = mixed(core)

                @pl.when(core == 0)
                def _():
                    give_copy(0, 0).start()
            else:
                sums[0, 0, n] = mixed(0)
                sums[0, 1, n] = mixed(1)
                give_copy(0, n).start()
            if n == 1:
                @pl.when(core == 0)
                def _():
                    lend_copy.start()

    remote_rows(0)
    for role in (2, 3):
        pltpu.make_async_copy(
            x_hbm.at[sources[role]], x_buf.at[:, pl.ds(role * capacity, capacity)], stream_sem.at[half]).start()
    remote_sums(0)

    def send_first():
        @pl.when(core == 0)
        def _():
            with jax.named_scope("send_on"):
                send_on(0)

    remote_rows(1, send_first)
    remote_sums(1)

    @pl.when(core == 1)
    def _():
        with jax.named_scope("send_on"):
            send_on(0)

    last = chunks - 1
    last = chunks - 1

    def last_remote_chunk():
        remote_rows(last)
        remote_sums(last)

    for n in range(2, last):
        remote_rows(n)
        remote_sums(n)
        with jax.named_scope("send_on"):
            send_on(n - 1)

    down_copy(last).wait()
    @pl.when(chip == 1)
    def _():
        last_remote_chunk()
        with jax.named_scope("send_on"):
            send_on(last - 1)

    local_rows = x_buf.at[:, pl.ds(pair, pair)]
    pltpu.make_async_copy(local_rows, local_rows, stream_sem.at[half]).wait()

    def local_step(e, carry):
        hidden(2, e)
        return carry

    def local_chunk(n):
        with jax.named_scope("rows2"):
            for e in range(experts):
                rows_of(2, n, e)
        with jax.named_scope("mixed2"):
            sums[1, 0, n] = mixed(2)
            sums[1, 1, n] = mixed(3)
            give_copy(1, n).start()

    lax.fori_loop(0, 3, local_step, 0)
    with jax.named_scope("send_on"):
        @pl.when(chip == 0)
        def _():
            send_on(last - 1)

        @pl.when(chip == 1)
        def _():
            send_on(last)
    with jax.named_scope("phase1L"):
        lax.fori_loop(3, experts, local_step, 0)
    for role in (2, 3):
        build_mix(role)
    local_chunk(last)

    @pl.when(chip == 0)
    def _():
        last_remote_chunk()

    with jax.named_scope("away"):
        @pl.when(lends_last)
        def _():
            give_copy(1, last).wait_recv()
            away_out[...] = sums[1, 1, last, 0:AWAY] + from_peer[1, last, 0:AWAY]
            away_copy.start()

    local_chunk(0)

    @pl.when(chip == 0)
    def _():
        with jax.named_scope("send_on"):
            send_on(last)

    for n in range(1, last - 1):
        local_chunk(n)

    with jax.named_scope("away_add"):
        @pl.when(adds_last)
        def _():
            away_copy.wait_recv()
            final_out[...] = (away_in[...] + link_out[last, 0:AWAY]).astype(jnp.bfloat16)
            final_copy.start()

    local_chunk(last - 1)

    @pl.when(jnp.logical_not(lends_last))
    def _():
        give_copy(1, last).wait_recv()

    with jax.named_scope("fin_give"):
        given = from_peer.at[1, pl.ds(0, last)]
        pltpu.make_async_remote_copy(
            src_ref=given, dst_ref=given, send_sem=send_sem, recv_sem=give_recv.at[chunks],
            device_id=(group, partner), device_id_type=MESH).wait_recv()

    with jax.named_scope("fin_side"):
        @pl.when(core == 0)
        def _():
            pltpu.make_async_remote_copy(
                src_ref=side_in, dst_ref=side_in, send_sem=send_sem, recv_sem=side_recv,
                device_id=(group, far), device_id_type=MESH).wait_recv()
            link_in[0, 0:DIRECT] = side_in[0:DIRECT] + side_in[DIRECT:2 * DIRECT]
            link_in[1, 0:LENT] = side_in[2 * DIRECT:]

        @pl.when(core == 1)
        def _():
            both = link_in.at[0, pl.ds(0, DIRECT + LENT)]
            pltpu.make_async_remote_copy(
                src_ref=both, dst_ref=both, send_sem=send_sem, recv_sem=side_recv,
                device_id=(group, far), device_id_type=MESH).wait_recv()

    for n in range(chunks):
        near = sums[1, 1, n] + from_peer[1, n]
        with jax.named_scope("fin_link"):
            if n == 0:
                count = ((chunks - 1) * tokens - DIRECT - LENT) // chunks
                part = link_in.at[:, pl.ds(0, count)]
                pltpu.make_async_remote_copy(
                    src_ref=part, dst_ref=part, send_sem=send_sem, recv_sem=link_recv.at[0],
                    device_id=(group, far), device_id_type=MESH).wait_recv()
        if n < last:
            out_ref[:, pl.ds(n * CHUNK, CHUNK)] = (near + link_in[n]).astype(jnp.bfloat16)
    cols = pl.ds(last * CHUNK, CHUNK)

    @pl.when(lends_last)
    def _():
        final_copy.wait_recv()
        out_ref[0:AWAY, cols] = final_in[...]
        with jax.named_scope("fin_last"):
            last_copy(AWAY).wait_recv()
        out_ref[AWAY:, cols] = (near[AWAY:] + link_in[last, AWAY:]).astype(jnp.bfloat16)

    @pl.when(jnp.logical_not(lends_last))
    def _():
        with jax.named_scope("fin_last"):
            last_copy(0).wait_recv()
        out_ref[:, cols] = (near + link_in[last]).astype(jnp.bfloat16)

    with jax.named_scope("w_send"):
        def wait_sent(ref):
            pltpu.make_async_remote_copy(
                src_ref=ref, dst_ref=ref, send_sem=send_sem, recv_sem=side_recv,
                device_id=(group, far), device_id_type=MESH).wait_send()

        wait_sent(route_in)
        wait_sent(from_peer)
        for n in range(last):
            link_copy(n).wait_send()
        @pl.when(lends_last)
        def _():
            away_copy.wait_send()

        @pl.when(adds_last)
        def _():
            last_copy(AWAY).wait_send()
            final_copy.wait_send()

        @pl.when(jnp.logical_not(adds_last))
        def _():
            last_copy(0).wait_send()
        direct_copy.wait_send()

        @pl.when(core == 0)
        def _():
            lend_copy.wait_send()

        @pl.when(core == 1)
        def _():
            for copy in (rest_copy, own_copy, lent_copy):
                copy.wait_send()


def solution(mesh):
    def local_step(dispatched, w_gate, w_up, w_down, fill_count, slot_index, expert_id, gate_weight):
        sources, experts, capacity, width = dispatched.shape
        ffn = w_gate.shape[2]
        tokens, choices = slot_index.shape
        chunks = width // CHUNK
        f32, bf16 = jnp.float32, jnp.bfloat16
        scratch = [
            pltpu.VMEM((experts, sources * capacity, width), bf16),
            pltpu.VMEM((experts, 2, width, ffn), bf16),
            pltpu.VMEM((experts, ffn, width), bf16),
            pltpu.SMEM((sources, experts), jnp.int32),
            pltpu.VMEM((2, choices, tokens), jnp.int32),
            pltpu.VMEM((choices, tokens), f32),
            pltpu.VMEM((2 * choices, tokens), f32),
            pltpu.VMEM((3, 2 * choices, tokens), f32),
            pltpu.VMEM((4, 3 * tokens, experts * capacity), bf16),
            pltpu.VMEM((experts, sources * capacity, ffn), bf16),
            pltpu.VMEM((2, experts * capacity, CHUNK), bf16),
            pltpu.VMEM((2, 2, chunks, tokens, CHUNK), f32),
            pltpu.VMEM((2, chunks, tokens, CHUNK), f32),
            pltpu.VMEM((chunks, tokens, CHUNK), f32),
            pltpu.VMEM((chunks, tokens, CHUNK), f32),
            pltpu.VMEM((2 * DIRECT + LENT, CHUNK), f32),
            pltpu.VMEM((LENT, CHUNK), f32),
            pltpu.VMEM((LENT, CHUNK), f32),
            pltpu.VMEM((AWAY, CHUNK), f32),
            pltpu.VMEM((AWAY, CHUNK), f32),
            pltpu.VMEM((AWAY, CHUNK), bf16),
            pltpu.VMEM((AWAY, CHUNK), bf16),
            pltpu.SemaphoreType.DMA((experts,)),
            pltpu.SemaphoreType.DMA((4,)),
            pltpu.SemaphoreType.DMA,
            pltpu.SemaphoreType.DMA,
            pltpu.SemaphoreType.DMA((chunks + 2,)),
            pltpu.SemaphoreType.DMA((2,)),
            pltpu.SemaphoreType.DMA,
            pltpu.SemaphoreType.DMA,
            pltpu.SemaphoreType.DMA,
        ]
        operands = (dispatched, w_gate, w_up, w_down, fill_count, slot_index.T, expert_id.T, gate_weight.T)
        return pl.pallas_call(
            kernel,
            out_shape=pltpu.VMEM((tokens, width), bf16),
            in_specs=[pl.BlockSpec(memory_space=pl.ANY)] * len(operands),
            out_specs=pl.BlockSpec(memory_space=pltpu.VMEM),
            scratch_shapes=scratch,
            compiler_params=pltpu.CompilerParams(
                collective_id=0, has_side_effects=True, vmem_limit_bytes=44 * 1024 * 1024),
            name="expert_return",
        )(*(pltpu.with_memory_space_constraint(array, pltpu.HBM) for array in operands))

    token_spec = P(("dp", "ep"))
    in_specs = (P("dp", "ep"), P("ep"), P("ep"), P("ep"), P("dp", "ep"), token_spec, token_spec, token_spec)
    return jax.shard_map(local_step, mesh=mesh, in_specs=in_specs, out_specs=token_spec, check_vma=False)
```
